32 devices in a mesh: tp: 4 (over z), ep: 8 (over y, x, core).
Axes of the slice: x: 2, y: 2, z: 4, core: 2. Of those that a mesh axis runs over, the one named last changes fastest.
Arguments:
- tokens: bfloat16 [3072, 2048], P('ep', 'tp'), may hold values from -6 to 6
- norm_gain: float32 [2048], replicated, may hold values from 0.25 to 1.75
- shared_gate: bfloat16 [2048, 2816], P('ep', 'tp'), may hold values from -0.125 to 0.125
- shared_up: bfloat16 [2048, 2816], P('ep', 'tp'), may hold values from -0.125 to 0.125
- shared_down: bfloat16 [2816, 2048], P('tp', 'ep'), may hold values from -0.15625 to 0.15625
- expert_gate: bfloat16 [4, 8, 704, 2048], P('tp', 'ep'), may hold values from -0.125 to 0.125
- expert_up: bfloat16 [4, 8, 704, 2048], P('tp', 'ep'), may hold values from -0.125 to 0.125
- expert_down: bfloat16 [16, 1408, 2048], P('ep', None, 'tp'), may hold values from -0.15625 to 0.15625
- chosen: int32 [16, 384], P('ep'), may hold values from 0 to 3071, as said below
- gates: float32 [16, 384], P('ep'), may hold values from 0.1 to 1
Outputs:
- mixed: bfloat16 [3072, 2048], P('ep', 'tp')
The draws below stay inside these ranges and needn't reach their ends.
Inputs may be any that keep to these rules, and one draw needn't show every extreme that they name: Each row of chosen holds 384 different token indices in rising order. Of one row, at most 96 lie among the 384 tokens of one index of ep (tokens s * 384 to (s + 1) * 384 - 1), and in every row exactly 96 lie among those of some index.
All inputs are finite; a program needn't handle non-finite values.
Results may differ from the reference program's by a relative error of at most 0.012.
Values may be sent and summed in bfloat16 or wider, within the bound.
A program may use at most 64 MiB of HBM per device.

```python
import jax
import jax.numpy as jnp
from jax import lax

D = 2048
FS = 2816
F = 1408
EXP_DEV = 2
TOK_DEV = 384
TOKENS = 3072
EXPERTS = 16
SPLIT = 2
CAP = 384
N_TP = 4
N_EP = 8


def expert_choices(expert_key):
    key_pair, key_shift, key_rank = jax.random.split(expert_key, 3)
    halves = N_EP // 2
    average = CAP // N_EP
    pairing = jax.random.permutation(key_pair, N_EP)
    shifts = jax.random.randint(key_shift, (halves,), 0, average + 1).astype(jnp.int32)
    shifts = shifts.at[0].set(average)
    counts = jnp.full((N_EP,), average, jnp.int32)
    counts = counts.at[pairing[:halves]].add(shifts).at[pairing[halves:]].add(-shifts)
    rank_keys = jax.random.split(key_rank, N_EP)
    rankings = jax.vmap(source_ranking)(rank_keys)
    flags = (rankings < counts[:, None]).reshape(-1).astype(jnp.int32)
    places = jnp.cumsum(flags) - 1
    places = jnp.where(flags > 0, places, CAP)
    token_ids = jnp.arange(N_EP * TOK_DEV, dtype=jnp.int32)
    return jnp.zeros((CAP,), jnp.int32).at[places].set(token_ids, mode='drop')


def source_ranking(rank_key):
    return jax.random.permutation(rank_key, TOK_DEV).astype(jnp.int32)


def draw_chosen(key, part):
    expert_keys = jax.random.split(jax.random.fold_in(key, 11), EXPERTS)
    return jax.vmap(expert_choices)(expert_keys)


def strengthened(array, own_key, source, target, shards_of, factor):
    owner, partner = [(jnp.arange(array.shape[position]) // (array.shape[position] // shards_of)).reshape([-1 if axis == position else 1 for axis in range(array.ndim)]) for position in (source, target)]
    chosen = jax.random.permutation(own_key, shards_of)[partner]
    strong = (owner == chosen) | (owner == (partner + shards_of // 2) % shards_of)
    return jnp.where(strong, factor * array, array)


def levels(stream_key, dims, cuts, low, top_value):
    def one(axis_at, shards_of):
        draws = jax.random.uniform(jax.random.fold_in(jax.random.fold_in(stream_key, 6), axis_at), (shards_of,), jnp.float32, low / len(cuts), top_value / len(cuts))
        return jnp.repeat(jnp.exp(draws), dims[axis_at] // shards_of).reshape((-1,) + (1,) * (len(dims) - axis_at - 1))

    level = one(*cuts[0])
    for cut in cuts[1:]:
        level = level * one(*cut)
    return level


def normal_values(key, shape, scale, most, cuts=(), held_as=jnp.bfloat16):
    entries = jax.random.normal(key, shape, jnp.float32) * scale
    if len(cuts) > 0:
        entries = levels(key, shape, cuts, -0.22, 0.18) * entries
    return jnp.clip(entries, min=-most, max=most).astype(held_as)


def bell_draw_with(own_key, extent, scale, reach, cuts, heavy, held_as=jnp.bfloat16):
    entries = scale * jax.random.normal(own_key, extent, jnp.float32)
    if cuts:
        entries = entries * levels(own_key, extent, cuts, -0.22, 0.18)
    return jnp.clip(strengthened(entries, jax.random.fold_in(own_key, 3), *heavy), -reach, reach).astype(held_as)


def setup_inputs(seed: int = 0) -> dict:
    key_list = jax.random.split(jax.random.key(seed), 11)
    tokens = normal_values(key_list[0], (TOKENS, D), 1.0, 6.0, ((0, 8), (1, 4)))
    norm_gain = jnp.clip(1.0 + 0.15 * jax.random.normal(key_list[1], (D,), jnp.float32), 0.25, 1.75)
    shared_gate = normal_values(key_list[2], (D, FS), D ** -0.5, 0.125, ((0, 8), (1, 4)))
    shared_up = normal_values(key_list[3], (D, FS), D ** -0.5, 0.125, ((0, 8), (1, 4)))
    shared_down = bell_draw_with(key_list[4], (FS, D), FS ** -0.5, 0.15625, ((0, 4), (1, 8)), (0, 1, 8, 2.0))
    expert_gate = normal_values(key_list[5], (N_TP, N_EP, F // SPLIT, D), D ** -0.5, 0.125, ((0, 4), (1, 8)))
    expert_up = normal_values(key_list[6], (N_TP, N_EP, F // SPLIT, D), D ** -0.5, 0.125, ((0, 4), (1, 8)))
    expert_down = normal_values(key_list[7], (EXPERTS, F, D), F ** -0.5, 0.15625, ((0, 8), (2, 4)))
    chosen = draw_chosen(jax.random.fold_in(key_list[10], 71), 0)
    gates = jnp.clip(0.1 + 0.9 * jax.random.uniform(key_list[9], (EXPERTS, CAP), jnp.float32) ** levels(key_list[9], (EXPERTS, CAP), ((0, 8),), -0.2, 0.2), 0.1, 1.0)
    return dict(tokens=tokens, norm_gain=norm_gain, shared_gate=shared_gate, shared_up=shared_up, shared_down=shared_down, expert_gate=expert_gate, expert_up=expert_up, expert_down=expert_down, chosen=chosen, gates=gates)


norm_eps = 1e-06

def reference(tokens, norm_gain, shared_gate, shared_up, shared_down, expert_gate, expert_up, expert_down, chosen, gates):
    widened = tokens.astype(jnp.float32)
    inv_scale = lax.rsqrt(lax.optimization_barrier(jnp.mean(widened * widened, axis=1, keepdims=True)) + norm_eps)
    normed = (widened * inv_scale * norm_gain.astype(jnp.float32)).astype(jnp.bfloat16)
    gate_sum = jnp.dot(normed, shared_gate, preferred_element_type=jnp.float32)
    up_sum = jnp.dot(normed, shared_up, preferred_element_type=jnp.float32)
    shared_hidden = (jax.nn.silu(gate_sum) * up_sum).astype(jnp.bfloat16)
    shared_out = jnp.dot(shared_hidden, shared_down, preferred_element_type=jnp.float32)
    split_count = N_TP // EXP_DEV

    def expert_term(expert_index):
        ep_column = (expert_index // EXP_DEV).astype(jnp.int32)
        expert_slot = (expert_index % EXP_DEV).astype(jnp.int32)

        def weight_of(weights):
            picked = lax.dynamic_index_in_dim(weights, ep_column, 1, keepdims=False)
            picked = lax.dynamic_slice_in_dim(picked, expert_slot * split_count, split_count, 0)
            return jnp.transpose(picked.reshape(F, D))
        token_ids = lax.dynamic_index_in_dim(chosen, expert_index, 0, keepdims=False)
        token_rows = jnp.take(normed, token_ids, axis=0)
        gate_values = jnp.dot(token_rows, weight_of(expert_gate), preferred_element_type=jnp.float32)
        up_values = jnp.dot(token_rows, weight_of(expert_up), preferred_element_type=jnp.float32)
        hidden = (jax.nn.silu(gate_values) * up_values).astype(jnp.bfloat16)
        down_weight = lax.dynamic_index_in_dim(expert_down, expert_index, 0, keepdims=False)
        outputs = jnp.dot(hidden, down_weight, preferred_element_type=jnp.float32)
        gate_row = lax.dynamic_index_in_dim(gates, expert_index, 0, keepdims=False).astype(jnp.float32)
        return (gate_row[:, None] * outputs).astype(jnp.bfloat16)
    weighted = lax.map(expert_term, jnp.arange(EXPERTS, dtype=jnp.int32))
    routed = jnp.zeros((TOKENS, D), jnp.float32).at[chosen.reshape(-1)].add(weighted.reshape(-1, D).astype(jnp.float32))
    return (shared_out + routed).astype(jnp.bfloat16)
```

```python
import functools

import jax
import jax.numpy as jnp
from jax import lax
from jax.experimental import pallas as pl
from jax.experimental.pallas import tpu as pltpu
from jax.sharding import PartitionSpec as P

norm_eps = 1e-06
MESH = pl.DeviceIdType.MESH


def flip(index, mask):
    bit = 1
    result = index
    while bit <= mask:
        if mask & bit:
            result = result + bit - 2 * bit * ((index // bit) % 2)
        bit *= 2
    return result


def bits_below(count):
    return [1 << i for i in range(count.bit_length() - 1)]


def half_orders(count):
    bits = bits_below(count)
    upper = bits[1:]
    return [upper + bits[:1], upper[::-1] + bits[:1]]


def later_hops(mask, order):
    last = max([i for i, b in enumerate(order) if mask & b], default=-1)
    return order[last + 1 :]


def masks_by_level(count):
    return sorted(range(1, count), key=lambda m: (bin(m).count("1"), -m))


def levels(count):
    found = {}
    for m in masks_by_level(count):
        found.setdefault(bin(m).count("1"), []).append(m)
    return [found[k] for k in sorted(found)]


def gather_kernel(
    n_tp,
    n_ep,
    tok_ref,
    sg_ref,
    su_ref,
    sd_ref,
    chosen_ref,
    sg_out,
    su_out,
    sd_out,
    own_out,
    used_out,
    tok_all,
    sel,
    total,
    ep_send,
    ep_recv,
    tp_send,
    tp_recv,
    disp_send,
    disp_recv,
    local_sem,
):
    tp = lax.axis_index("tp")
    ep = lax.axis_index("ep")
    n_exp, cap = chosen_ref.shape[0], chosen_ref.shape[1]
    n_tok, width = tok_ref.shape
    split = n_tp // n_exp
    slot = tp // split
    orders = half_orders(n_ep)
    high_masks = [k * split for k in range(1, n_exp)]
    tp_bits = bits_below(n_tp)
    tp_order = tp_bits[::-1]
    tp_partners = sorted(set(tp_bits) | set(high_masks))

    barrier = pltpu.get_barrier_semaphore()
    for b in bits_below(n_ep):
        pl.semaphore_signal(barrier, inc=1, device_id={"ep": flip(ep, b)}, device_id_type=MESH)
    for b in tp_partners:
        pl.semaphore_signal(barrier, inc=1, device_id={"tp": flip(tp, b)}, device_id_type=MESH)
    pl.semaphore_wait(barrier, len(bits_below(n_ep)) + len(tp_partners))

    def block_of(out, block, rows):
        if len(out.shape) == 3:
            return out.at[block, rows, :]
        cols = out.shape[1] // n_ep
        return out.at[rows, pl.ds(pl.multiple_of(block * cols, cols), cols)]

    def sources(w):
        return [tok_ref, sg_ref, su_ref, sd_ref][w]

    def own_piece(w, h):
        ref = sources(w)
        half = ref.shape[0] // 2
        return ref.at[pl.ds(h * half, half), :]

    def piece(w, block, h):
        ref = sources(w)
        half = ref.shape[0] // 2
        if w == 0:
            return tok_all.at[block, pl.ds(h * half, half), :]
        return block_of([None, sg_out, su_out, sd_out][w], block, pl.ds(h * half, half))

    def ep_copy(w, h, mask, hop):
        return pltpu.make_async_remote_copy(
            src_ref=own_piece(w, h) if mask == 0 else piece(w, flip(ep, mask), h),
            dst_ref=piece(w, flip(ep, mask), h),
            send_sem=ep_send.at[w, h, mask | hop],
            recv_sem=ep_recv.at[w, h, mask | hop],
            device_id={"ep": flip(ep, hop)},
            device_id_type=MESH,
        )

    def ep_arrival(w, h, mask):
        order = orders[h]
        hop = [b for b in order if mask & b][-1]
        dst = piece(w, flip(ep, mask), h)
        return pltpu.make_async_remote_copy(
            src_ref=dst,
            dst_ref=dst,
            send_sem=ep_send.at[w, h, mask],
            recv_sem=ep_recv.at[w, h, mask],
            device_id={"ep": flip(ep, hop)},
            device_id_type=MESH,
        )

    def ep_start(w):
        for position in range(len(orders[0])):
            for h in (0, 1):
                ep_copy(w, h, 0, orders[h][position]).start()

    def ep_level(w, masks):
        for mask in masks:
            for h in (0, 1):
                ep_arrival(w, h, mask).wait_recv()
                for hop in later_hops(mask, orders[h]):
                    ep_copy(w, h, mask, hop).start()

    def columns(ref, block):
        return ref.at[:, pl.ds(pl.multiple_of(block * width, width), width)]

    def tp_copy(mask, hop):
        return pltpu.make_async_remote_copy(
            src_ref=tok_ref if mask == 0 else columns(own_out, flip(tp, mask)),
            dst_ref=columns(own_out, flip(tp, mask)),
            send_sem=tp_send.at[mask | hop],
            recv_sem=tp_recv.at[mask | hop],
            device_id={"tp": flip(tp, hop)},
            device_id_type=MESH,
        )

    def disp_copy(mask, hop):
        if mask == 0:
            src = sel.at[flip(tp, hop) // split]
        else:
            src = columns(used_out, flip(tp, mask))
        return pltpu.make_async_remote_copy(
            src_ref=src,
            dst_ref=columns(used_out, flip(tp, mask)),
            send_sem=disp_send.at[mask | hop],
            recv_sem=disp_recv.at[mask | hop],
            device_id={"tp": flip(tp, hop)},
            device_id_type=MESH,
        )

    def low_hops(mask):
        low = mask % split
        return [b for b in bits_below(split) if b > low]

    def local_copies():
        items = [(0, tok_ref, tok_all.at[ep]), (1, tok_ref, columns(own_out, tp))]
        pairs = ((sg_ref, sg_out), (su_ref, su_out), (sd_ref, sd_out))
        for i, (ref, out) in enumerate(pairs):
            items.append((2 + i, ref, block_of(out, ep, pl.ds(0, ref.shape[0]))))
        return [pltpu.make_async_copy(s, d, local_sem.at[i]) for i, s, d in items]

    ep_start(0)
    tp_copy(0, tp_order[0]).start()
    locals_started = local_copies()
    for copy in locals_started:
        copy.start()
    ep_levels = levels(n_ep)
    ep_level(0, ep_levels[0])
    for w in (1, 2, 3):
        ep_start(w)
    for masks in ep_levels[1:]:
        ep_level(0, masks)
    locals_started[0].wait()

    for s in range(n_exp):
        total[...] = jnp.zeros_like(total)

        def add_source(e, carry):
            ids = lax.broadcasted_iota(jnp.int32, (cap, n_tok), 1) + e * n_tok
            hits = jnp.where(chosen_ref[s] == ids, 1.0, 0.0).astype(jnp.bfloat16)
            total[...] += jnp.dot(hits, tok_all[e], preferred_element_type=jnp.float32)
            return carry

        lax.fori_loop(0, n_ep, add_source, 0)
        sel[s] = total[...].astype(jnp.bfloat16)

    for mask in high_masks:
        disp_copy(0, mask).start()
    for hop in low_hops(0):
        disp_copy(0, hop).start()
    own_used = pltpu.make_async_copy(sel.at[slot], columns(used_out, tp), local_sem.at[5])
    own_used.start()

    for w in (1, 2, 3):
        ep_level(w, ep_levels[0])
    for mask in high_masks:
        disp_wait(
            columns(used_out, flip(tp, mask)), disp_send, disp_recv, mask, tp
        )
        for hop in low_hops(mask):
            disp_copy(mask, hop).start()
    for hop in tp_order[1:]:
        tp_copy(0, hop).start()
    tp_seen = []
    for mask in sorted(range(1, n_tp), key=lambda m: [tp_order.index(b) for b in tp_order if m & b][-1]):
        last = [b for b in tp_order if mask & b][-1]
        if last == tp_order[0]:
            disp_wait(columns(own_out, flip(tp, mask)), tp_send, tp_recv, mask, tp)
            tp_seen.append(mask)
            for hop in later_hops(mask, tp_order):
                tp_copy(mask, hop).start()
    for masks in ep_levels[1:]:
        for w in (1, 2, 3):
            ep_level(w, masks)
    for mask in range(1, n_tp):
        if mask not in high_masks:
            disp_wait(columns(used_out, flip(tp, mask)), disp_send, disp_recv, mask, tp)
            for hop in low_hops(mask):
                disp_copy(mask, hop).start()
    for mask in sorted(range(1, n_tp), key=lambda m: [tp_order.index(b) for b in tp_order if m & b][-1]):
        if mask not in tp_seen:
            disp_wait(columns(own_out, flip(tp, mask)), tp_send, tp_recv, mask, tp)
            for hop in later_hops(mask, tp_order):
                tp_copy(mask, hop).start()

    for copy in locals_started[1:]:
        copy.wait()
    own_used.wait()
    for w in range(4):
        for h in (0, 1):
            for mask in range(n_ep):
                for hop in later_hops(mask, orders[h]):
                    ep_copy(w, h, mask, hop).wait_send()
    for mask in range(n_tp):
        for hop in later_hops(mask, tp_order):
            tp_copy(mask, hop).wait_send()
    for mask in [0] + high_masks + [m for m in range(1, n_tp) if m not in high_masks]:
        hops = low_hops(mask)
        if mask == 0:
            hops = high_masks + hops
        for hop in hops:
            disp_copy(mask, hop).wait_send()


def disp_wait(dst, send_sem, recv_sem, mask, tp):
    pltpu.make_async_remote_copy(
        src_ref=dst,
        dst_ref=dst,
        send_sem=send_sem.at[mask],
        recv_sem=recv_sem.at[mask],
        device_id={"tp": flip(tp, mask)},
        device_id_type=MESH,
    ).wait_recv()


def upfront(n_tp, n_ep, tokens, shared_gate, shared_up, shared_down, chosen):
    n_tok, width = tokens.shape
    n_exp, cap = chosen.shape
    vmem = pl.BlockSpec(memory_space=pltpu.VMEM)
    hbm = pl.BlockSpec(memory_space=pl.ANY)
    bf16 = jnp.bfloat16

    def joined(weight):
        rows, cols = weight.shape
        if cols % 128 == 0:
            return jax.ShapeDtypeStruct((rows, n_ep * cols), bf16)
        return jax.ShapeDtypeStruct((n_ep, rows, cols), bf16)

    return pl.pallas_call(
        functools.partial(gather_kernel, n_tp, n_ep),
        out_shape=(
            joined(shared_gate),
            joined(shared_up),
            joined(shared_down),
            jax.ShapeDtypeStruct((n_tok, n_tp * width), bf16),
            jax.ShapeDtypeStruct((cap, n_tp * width), bf16),
        ),
        in_specs=[vmem] * 5,
        out_specs=(hbm,) * 5,
        scratch_shapes=[
            pltpu.VMEM((n_ep, n_tok, width), bf16),
            pltpu.VMEM((n_exp, cap, width), bf16),
            pltpu.VMEM((cap, width), jnp.float32),
            pltpu.SemaphoreType.DMA((4, 2, n_ep)),
            pltpu.SemaphoreType.DMA((4, 2, n_ep)),
            pltpu.SemaphoreType.DMA((n_tp,)),
            pltpu.SemaphoreType.DMA((n_tp,)),
            pltpu.SemaphoreType.DMA((n_tp,)),
            pltpu.SemaphoreType.DMA((n_tp,)),
            pltpu.SemaphoreType.DMA((6,)),
        ],
        compiler_params=pltpu.CompilerParams(
            collective_id=0, has_side_effects=True, vmem_limit_bytes=48 * 1024 * 1024
        ),
    )(tokens, shared_gate, shared_up, shared_down, chosen[:, :, None])


def flat_weight(weight):
    if weight.ndim == 2:
        return weight
    return jnp.moveaxis(weight, 0, 1).reshape(weight.shape[1], -1)


def normalise(rows, gain):
    widened = rows.astype(jnp.float32)
    inv_scale = lax.rsqrt(jnp.mean(widened * widened, axis=1, keepdims=True) + norm_eps)
    return (widened * inv_scale * gain).astype(jnp.bfloat16)


def swap_tp(value, n_tp, mask):
    return lax.ppermute(value, "tp", [(i, i ^ mask) for i in range(n_tp)])


def gather_tp(block, n_tp):
    tp = lax.axis_index("tp")
    held = block[None]
    for bit in bits_below(n_tp)[::-1]:
        other = swap_tp(held, n_tp, bit)
        upper = (tp // bit) % 2 == 1
        first = jnp.where(upper, other, held)
        second = jnp.where(upper, held, other)
        held = jnp.stack([first, second], axis=1).reshape((-1,) + block.shape)
    return held


def scatter_sum_tp(partial, n_tp):
    tp = lax.axis_index("tp")
    rows = partial.shape[0]
    width = partial.shape[1] // n_tp
    blocks = [partial[:, i * width : (i + 1) * width] for i in range(n_tp)]
    for bit in bits_below(n_tp):
        upper = (tp // bit) % 2 == 1
        send = [jnp.where(upper, blocks[i], blocks[i + 1]) for i in range(0, len(blocks), 2)]
        keep = [jnp.where(upper, blocks[i + 1], blocks[i]) for i in range(0, len(blocks), 2)]
        got = swap_tp(jnp.stack(send).astype(jnp.bfloat16), n_tp, bit)
        blocks = [k + got[i].astype(jnp.float32) for i, k in enumerate(keep)]
    return blocks[0]


def on_device(
    tokens,
    norm_gain,
    shared_gate,
    shared_up,
    shared_down,
    expert_gate,
    expert_up,
    expert_down,
    chosen,
    gates,
):
    n_tp = lax.axis_size("tp")
    n_ep = lax.axis_size("ep")
    ep = lax.axis_index("ep")
    n_exp, cap = chosen.shape
    n_tok, width = tokens.shape
    f32 = jnp.float32

    all_chosen = lax.all_gather(chosen, "ep", axis=0, tiled=True)
    sg, su, sd, own_rows, used_rows = upfront(
        n_tp, n_ep, tokens, shared_gate.T, shared_up.T, shared_down, chosen
    )
    sg, su, sd = flat_weight(sg), flat_weight(su), flat_weight(sd)

    slot_most = 2 * cap // n_ep
    positions = jnp.arange(cap, dtype=jnp.int32)
    sources = chosen // n_tok
    before = chosen[:, None, :] < (sources * n_tok)[:, :, None]
    run_start = jnp.sum(before.astype(jnp.int32), axis=2)
    slot_index = sources * slot_most + positions[None, :] - run_start
    first = jnp.sum((all_chosen < ep * n_tok).astype(jnp.int32), axis=1)
    stop = jnp.sum((all_chosen < (ep + 1) * n_tok).astype(jnp.int32), axis=1)
    slots = jnp.arange(slot_most, dtype=jnp.int32)
    wanted = first[:, None] + slots[None, :]
    wanted = jnp.where(wanted < stop[:, None], wanted, -1)
    own_ids = jnp.sum(
        jnp.where(
            wanted[:, :, None] == positions[None, None, :],
            (all_chosen - ep * n_tok + 1)[:, None, :],
            0,
        ),
        axis=2,
    ) - 1

    used = normalise(used_rows, norm_gain)
    gate_weight = expert_gate.reshape(expert_gate.shape[2], expert_gate.shape[3])
    up_weight = expert_up.reshape(expert_up.shape[2], expert_up.shape[3])
    gate_values = jnp.einsum("hd,rd->hr", gate_weight, used, preferred_element_type=f32)
    up_values = jnp.einsum("hd,rd->hr", up_weight, used, preferred_element_type=f32)
    part_hidden = (jax.nn.silu(gate_values) * up_values).astype(jnp.bfloat16)
    all_hidden = gather_tp(part_hidden, n_tp)

    normed = normalise(own_rows, norm_gain)
    gate_sum = jnp.einsum("rd,hd->rh", normed, sg, preferred_element_type=f32)
    up_sum = jnp.einsum("rd,hd->rh", normed, su, preferred_element_type=f32)
    shared_hidden = (jax.nn.silu(gate_sum) * up_sum).astype(jnp.bfloat16)
    partial_out = jnp.dot(shared_hidden, sd, preferred_element_type=f32)
    shared_part = scatter_sum_tp(partial_out, n_tp)

    hidden = all_hidden.reshape(n_exp, expert_down.shape[1], cap)
    placed = []
    for s in range(n_exp):
        outputs = jnp.einsum("fr,fd->rd", hidden[s], expert_down[s], preferred_element_type=f32)
        weighted = (gates[s][:, None] * outputs).astype(jnp.bfloat16)
        placer = jnp.arange(n_ep * slot_most, dtype=jnp.int32)[:, None] == slot_index[s][None, :]
        placed.append(
            jnp.dot(placer.astype(jnp.bfloat16), weighted, preferred_element_type=f32)
            .astype(jnp.bfloat16)
            .reshape(n_ep, slot_most, width)
        )
    stacked = jnp.concatenate(placed, axis=1)
    returned = lax.all_to_all(stacked, "ep", split_axis=0, concat_axis=0, tiled=True)
    flat_values = returned.reshape(-1, width)
    flat_ids = own_ids.reshape(-1)
    picker = jnp.arange(n_tok, dtype=jnp.int32)[:, None] == flat_ids[None, :]
    routed = jnp.dot(picker.astype(jnp.bfloat16), flat_values, preferred_element_type=f32)
    return (shared_part + routed).astype(jnp.bfloat16)


def solution(mesh):
    return jax.shard_map(
        on_device,
        mesh=mesh,
        in_specs=(
            P("ep", "tp"),
            P(),
            P("ep", "tp"),
            P("ep", "tp"),
            P("tp", "ep"),
            P("tp", "ep", None, None),
            P("tp", "ep", None, None),
            P("ep", None, "tp"),
            P("ep", None),
            P("ep", None),
        ),
        out_specs=P("ep", "tp"),
        check_vma=False,
    )
```

```python
import functools

import jax
import jax.numpy as jnp
from jax import lax
from jax.experimental import pallas as pl
from jax.experimental.pallas import tpu as pltpu
from jax.sharding import PartitionSpec as P

norm_eps = 1e-06
MESH = pl.DeviceIdType.MESH


def flip(index, mask):
    bit = 1
    result = index
    while bit <= mask:
        if mask & bit:
            result = result + bit - 2 * bit * ((index // bit) % 2)
        bit *= 2
    return result


def bits_below(count):
    return [1 << i for i in range(count.bit_length() - 1)]


def half_orders(count):
    bits = bits_below(count)
    upper = bits[1:]
    return [upper + bits[:1], upper[::-1] + bits[:1]]


def later_hops(mask, order):
    last = max([i for i, b in enumerate(order) if mask & b], default=-1)
    return order[last + 1 :]


def masks_by_level(count):
    return sorted(range(1, count), key=lambda m: (bin(m).count("1"), -m))


def levels(count):
    found = {}
    for m in masks_by_level(count):
        found.setdefault(bin(m).count("1"), []).append(m)
    return [found[k] for k in sorted(found)]


def gather_kernel(
    n_tp,
    n_ep,
    tok_ref,
    sg_ref,
    su_ref,
    sd_ref,
    chosen_ref,
    ids_ref,
    sg_out,
    su_out,
    sd_out,
    own_out,
    used_out,
    ids_out,
    tok_all,
    sel,
    total,
    ep_send,
    ep_recv,
    tp_send,
    tp_recv,
    disp_send,
    disp_recv,
    local_sem,
):
    tp = lax.axis_index("tp")
    ep = lax.axis_index("ep")
    n_exp, cap = chosen_ref.shape[0], chosen_ref.shape[1]
    n_tok, width = tok_ref.shape
    split = n_tp // n_exp
    slot = tp // split
    orders = half_orders(n_ep)
    high_masks = [k * split for k in range(1, n_exp)]
    tp_bits = bits_below(n_tp)
    tp_order = tp_bits[::-1]
    tp_partners = sorted(set(tp_bits) | set(high_masks))

    barrier = pltpu.get_barrier_semaphore()
    for b in bits_below(n_ep):
        pl.semaphore_signal(barrier, inc=1, device_id={"ep": flip(ep, b)}, device_id_type=MESH)
    for b in tp_partners:
        pl.semaphore_signal(barrier, inc=1, device_id={"tp": flip(tp, b)}, device_id_type=MESH)
    pl.semaphore_wait(barrier, len(bits_below(n_ep)) + len(tp_partners))

    def block_of(out, block, rows):
        if len(out.shape) == 3:
            return out.at[block, rows, :]
        cols = out.shape[1] // n_ep
        return out.at[rows, pl.ds(pl.multiple_of(block * cols, cols), cols)]

    def sources(w):
        return [tok_ref, sg_ref, su_ref, sd_ref, ids_ref][w]

    def halves(w):
        return (0, 1) if w < 4 else (0,)

    def own_piece(w, h):
        ref = sources(w)
        if w == 4:
            return ref
        half = ref.shape[0] // 2
        return ref.at[pl.ds(h * half, half), :]

    def piece(w, block, h):
        ref = sources(w)
        if w == 4:
            return ids_out.at[block]
        half = ref.shape[0] // 2
        if w == 0:
            return tok_all.at[block, pl.ds(h * half, half), :]
        return block_of([None, sg_out, su_out, sd_out][w], block, pl.ds(h * half, half))

    def ep_copy(w, h, mask, hop):
        return pltpu.make_async_remote_copy(
            src_ref=own_piece(w, h) if mask == 0 else piece(w, flip(ep, mask), h),
            dst_ref=piece(w, flip(ep, mask), h),
            send_sem=ep_send.at[w, h, mask | hop],
            recv_sem=ep_recv.at[w, h, mask | hop],
            device_id={"ep": flip(ep, hop)},
            device_id_type=MESH,
        )

    def ep_arrival(w, h, mask):
        order = orders[h]
        hop = [b for b in order if mask & b][-1]
        dst = piece(w, flip(ep, mask), h)
        return pltpu.make_async_remote_copy(
            src_ref=dst,
            dst_ref=dst,
            send_sem=ep_send.at[w, h, mask],
            recv_sem=ep_recv.at[w, h, mask],
            device_id={"ep": flip(ep, hop)},
            device_id_type=MESH,
        )

    def ep_start(w):
        for position in range(len(orders[0])):
            for h in halves(w):
                ep_copy(w, h, 0, orders[h][position]).start()

    def ep_level(w, masks):
        for mask in masks:
            for h in halves(w):
                ep_arrival(w, h, mask).wait_recv()
                for hop in later_hops(mask, orders[h]):
                    ep_copy(w, h, mask, hop).start()

    def columns(ref, block):
        return ref.at[:, pl.ds(pl.multiple_of(block * width, width), width)]

    def tp_copy(mask, hop):
        return pltpu.make_async_remote_copy(
            src_ref=tok_ref if mask == 0 else columns(own_out, flip(tp, mask)),
            dst_ref=columns(own_out, flip(tp, mask)),
            send_sem=tp_send.at[mask | hop],
            recv_sem=tp_recv.at[mask | hop],
            device_id={"tp": flip(tp, hop)},
            device_id_type=MESH,
        )

    def disp_copy(mask, hop):
        if mask == 0:
            src = sel.at[flip(tp, hop) // split]
        else:
            src = columns(used_out, flip(tp, mask))
        return pltpu.make_async_remote_copy(
            src_ref=src,
            dst_ref=columns(used_out, flip(tp, mask)),
            send_sem=disp_send.at[mask | hop],
            recv_sem=disp_recv.at[mask | hop],
            device_id={"tp": flip(tp, hop)},
            device_id_type=MESH,
        )

    def low_hops(mask):
        low = mask % split
        return [b for b in bits_below(split) if b > low]

    def local_copies():
        items = [(0, tok_ref, tok_all.at[ep]), (6, ids_ref, ids_out.at[ep]), (1, tok_ref, columns(own_out, tp))]
        pairs = ((sg_ref, sg_out), (su_ref, su_out), (sd_ref, sd_out))
        for i, (ref, out) in enumerate(pairs):
            items.append((2 + i, ref, block_of(out, ep, pl.ds(0, ref.shape[0]))))
        return [pltpu.make_async_copy(s, d, local_sem.at[i]) for i, s, d in items]

    ep_start(0)
    tp_copy(0, tp_order[0]).start()
    locals_started = local_copies()
    for copy in locals_started:
        copy.start()
    ep_levels = levels(n_ep)
    ep_level(0, ep_levels[0])
    for w in (1, 2, 3, 4):
        ep_start(w)
    for masks in ep_levels[1:]:
        ep_level(0, masks)
    locals_started[0].wait()

    for s in range(n_exp):
        total[...] = jnp.zeros_like(total)

        def add_source(e, carry):
            ids = lax.broadcasted_iota(jnp.int32, (cap, n_tok), 1) + e * n_tok
            hits = jnp.where(chosen_ref[s] == ids, 1.0, 0.0).astype(jnp.bfloat16)
            total[...] += jnp.dot(hits, tok_all[e], preferred_element_type=jnp.float32)
            return carry

        lax.fori_loop(0, n_ep, add_source, 0)
        sel[s] = total[...].astype(jnp.bfloat16)

    for mask in high_masks:
        disp_copy(0, mask).start()
    for hop in low_hops(0):
        disp_copy(0, hop).start()
    own_used = pltpu.make_async_copy(sel.at[slot], columns(used_out, tp), local_sem.at[5])
    own_used.start()

    for w in (1, 2, 3, 4):
        ep_level(w, ep_levels[0])
    for mask in high_masks:
        disp_wait(
            columns(used_out, flip(tp, mask)), disp_send, disp_recv, mask, tp
        )
        for hop in low_hops(mask):
            disp_copy(mask, hop).start()
    for hop in tp_order[1:]:
        tp_copy(0, hop).start()
    tp_seen = []
    for mask in sorted(range(1, n_tp), key=lambda m: [tp_order.index(b) for b in tp_order if m & b][-1]):
        last = [b for b in tp_order if mask & b][-1]
        if last == tp_order[0]:
            disp_wait(columns(own_out, flip(tp, mask)), tp_send, tp_recv, mask, tp)
            tp_seen.append(mask)
            for hop in later_hops(mask, tp_order):
                tp_copy(mask, hop).start()
    for masks in ep_levels[1:]:
        for w in (1, 2, 3, 4):
            ep_level(w, masks)
    for mask in range(1, n_tp):
        if mask not in high_masks:
            disp_wait(columns(used_out, flip(tp, mask)), disp_send, disp_recv, mask, tp)
            for hop in low_hops(mask):
                disp_copy(mask, hop).start()
    for mask in sorted(range(1, n_tp), key=lambda m: [tp_order.index(b) for b in tp_order if m & b][-1]):
        if mask not in tp_seen:
            disp_wait(columns(own_out, flip(tp, mask)), tp_send, tp_recv, mask, tp)
            for hop in later_hops(mask, tp_order):
                tp_copy(mask, hop).start()

    for copy in locals_started[1:]:
        copy.wait()
    own_used.wait()
    for w in range(5):
        for h in halves(w):
            for mask in range(n_ep):
                for hop in later_hops(mask, orders[h]):
                    ep_copy(w, h, mask, hop).wait_send()
    for mask in range(n_tp):
        for hop in later_hops(mask, tp_order):
            tp_copy(mask, hop).wait_send()
    for mask in [0] + high_masks + [m for m in range(1, n_tp) if m not in high_masks]:
        hops = low_hops(mask)
        if mask == 0:
            hops = high_masks + hops
        for hop in hops:
            disp_copy(mask, hop).wait_send()


def disp_wait(dst, send_sem, recv_sem, mask, tp):
    pltpu.make_async_remote_copy(
        src_ref=dst,
        dst_ref=dst,
        send_sem=send_sem.at[mask],
        recv_sem=recv_sem.at[mask],
        device_id={"tp": flip(tp, mask)},
        device_id_type=MESH,
    ).wait_recv()


def upfront(n_tp, n_ep, tokens, shared_gate, shared_up, shared_down, chosen):
    n_tok, width = tokens.shape
    n_exp, cap = chosen.shape
    vmem = pl.BlockSpec(memory_space=pltpu.VMEM)
    hbm = pl.BlockSpec(memory_space=pl.ANY)
    bf16 = jnp.bfloat16

    def joined(weight):
        rows, cols = weight.shape
        if cols % 128 == 0:
            return jax.ShapeDtypeStruct((rows, n_ep * cols), bf16)
        return jax.ShapeDtypeStruct((n_ep, rows, cols), bf16)

    return pl.pallas_call(
        functools.partial(gather_kernel, n_tp, n_ep),
        out_shape=(
            joined(shared_gate),
            joined(shared_up),
            joined(shared_down),
            jax.ShapeDtypeStruct((n_tok, n_tp * width), bf16),
            jax.ShapeDtypeStruct((cap, n_tp * width), bf16),
            jax.ShapeDtypeStruct((n_ep, n_exp, cap), jnp.int32),
        ),
        in_specs=[vmem] * 6,
        out_specs=(hbm,) * 5 + (vmem,),
        scratch_shapes=[
            pltpu.VMEM((n_ep, n_tok, width), bf16),
            pltpu.VMEM((n_exp, cap, width), bf16),
            pltpu.VMEM((cap, width), jnp.float32),
            pltpu.SemaphoreType.DMA((5, 2, n_ep)),
            pltpu.SemaphoreType.DMA((5, 2, n_ep)),
            pltpu.SemaphoreType.DMA((n_tp,)),
            pltpu.SemaphoreType.DMA((n_tp,)),
            pltpu.SemaphoreType.DMA((n_tp,)),
            pltpu.SemaphoreType.DMA((n_tp,)),
            pltpu.SemaphoreType.DMA((7,)),
        ],
        compiler_params=pltpu.CompilerParams(
            collective_id=0, has_side_effects=True, vmem_limit_bytes=48 * 1024 * 1024
        ),
    )(tokens, shared_gate, shared_up, shared_down, chosen[:, :, None], chosen)


def flat_weight(weight):
    if weight.ndim == 2:
        return weight
    return jnp.moveaxis(weight, 0, 1).reshape(weight.shape[1], -1)


def normalise(rows, gain):
    widened = rows.astype(jnp.float32)
    inv_scale = lax.rsqrt(jnp.mean(widened * widened, axis=1, keepdims=True) + norm_eps)
    return (widened * inv_scale * gain).astype(jnp.bfloat16)


def finish_kernel(
    n_tp,
    n_ep,
    part_ref,
    normed_ref,
    sg_hbm,
    su_hbm,
    sd_hbm,
    down_hbm,
    gates_ref,
    place_ref,
    ids_ref,
    out_ref,
    sg_ref,
    su_ref,
    sd_ref,
    down_ref,
    hidden,
    acc,
    parts,
    parts_in,
    stage,
    back,
    load_sem,
    hid_send,
    hid_recv,
    sum_send,
    sum_recv,
    ret_send,
    ret_recv,
):
    tp = lax.axis_index("tp")
    ep = lax.axis_index("ep")
    n_tok, width = out_ref.shape
    n_exp = gates_ref.shape[0]
    split = n_tp // n_exp
    f32, bf16 = jnp.float32, jnp.bfloat16
    order = bits_below(n_tp)[::-1]
    half = part_ref.shape[0] // 2

    barrier = pltpu.get_barrier_semaphore()
    for mask in range(1, n_tp):
        pl.semaphore_signal(barrier, inc=1, device_id={"tp": flip(tp, mask)}, device_id_type=MESH)
    for mask in range(1, n_ep):
        pl.semaphore_signal(barrier, inc=1, device_id={"ep": flip(ep, mask)}, device_id_type=MESH)
    pl.semaphore_wait(barrier, n_tp + n_ep - 2)

    def hid_copy(mask, hop, h):
        rows = pl.ds(h * half, half)
        block = flip(tp, mask)
        return pltpu.make_async_remote_copy(
            src_ref=part_ref.at[rows, :] if mask == 0 else hidden.at[block, rows, :],
            dst_ref=hidden.at[block, rows, :],
            send_sem=hid_send.at[mask | hop, h],
            recv_sem=hid_recv.at[mask | hop, h],
            device_id={"tp": flip(tp, hop)},
            device_id_type=MESH,
        )

    def hid_arrived(mask, h):
        dst = hidden.at[flip(tp, mask), pl.ds(h * half, half), :]
        pltpu.make_async_remote_copy(
            src_ref=dst,
            dst_ref=dst,
            send_sem=hid_send.at[mask, h],
            recv_sem=hid_recv.at[mask, h],
            device_id={"tp": flip(tp, mask)},
            device_id_type=MESH,
        ).wait_recv()

    def sum_copy(mask):
        return pltpu.make_async_remote_copy(
            src_ref=parts.at[flip(tp, mask)],
            dst_ref=parts_in.at[mask],
            send_sem=sum_send.at[mask],
            recv_sem=sum_recv.at[mask],
            device_id={"tp": flip(tp, mask)},
            device_id_type=MESH,
        )

    def ret_copy(mask):
        return pltpu.make_async_remote_copy(
            src_ref=stage.at[flip(ep, mask)],
            dst_ref=back.at[ep],
            send_sem=ret_send.at[mask],
            recv_sem=ret_recv.at[mask],
            device_id={"ep": flip(ep, mask)},
            device_id_type=MESH,
        )

    def ret_arrived(mask):
        dst = back.at[flip(ep, mask)]
        pltpu.make_async_remote_copy(
            src_ref=dst,
            dst_ref=dst,
            send_sem=ret_send.at[mask],
            recv_sem=ret_recv.at[mask],
            device_id={"ep": flip(ep, mask)},
            device_id_type=MESH,
        ).wait_recv()

    for hop in order:
        for h in (0, 1):
            hid_copy(0, hop, h).start()
    pairs = ((sg_hbm, sg_ref), (su_hbm, su_ref), (sd_hbm, sd_ref), (down_hbm, down_ref))
    loads = [pltpu.make_async_copy(s, d, load_sem.at[i]) for i, (s, d) in enumerate(pairs)]
    for load in loads:
        load.start()

    for load in loads[:3]:
        load.wait()
    chunk = n_tok // 2

    def shared_rows(i, carry):
        rows = pl.ds(pl.multiple_of(i * chunk, chunk), chunk)
        x = normed_ref[rows, :]
        contract = (((1,), (1,)), ((), ()))
        gate = lax.dot_general(x, sg_ref[...], contract, preferred_element_type=f32)
        up = lax.dot_general(x, su_ref[...], contract, preferred_element_type=f32)
        mid = (jax.nn.silu(gate) * up).astype(bf16)
        for block in range(n_tp):
            cols = pl.ds(block * width, width)
            parts[block, rows, :] = jnp.dot(
                mid, sd_ref[:, cols], preferred_element_type=f32
            ).astype(bf16)
        return carry

    lax.fori_loop(0, 2, shared_rows, 0)
    loads[3].wait()

    acc[...] = jnp.zeros_like(acc)

    def add_block(mask):
        block = flip(tp, mask)
        value = part_ref[...] if mask == 0 else hidden[block]
        slot = block // split
        acc[slot] += lax.dot_general(
            value, down_ref[block], (((0,), (0,)), ((), ())), preferred_element_type=f32
        )

    arrivals = sorted(
        range(1, n_tp), key=lambda m: [order.index(b) for b in order if m & b][::-1]
    )
    tp_masks = list(range(1, n_tp))
    first_hop = [m for m in arrivals if m == order[0]]
    for mask in first_hop:
        for h in (0, 1):
            hid_arrived(mask, h)
            for hop in later_hops(mask, order):
                hid_copy(mask, hop, h).start()
    for mask in tp_masks:
        sum_copy(mask).start()
    add_block(0)
    for mask in first_hop:
        add_block(mask)
    for mask in arrivals:
        if mask in first_hop:
            continue
        for h in (0, 1):
            hid_arrived(mask, h)
            for hop in later_hops(mask, order):
                hid_copy(mask, hop, h).start()
        add_block(mask)

    slots = stage.shape[0] * stage.shape[2]
    for s in range(n_exp):
        weighted = (gates_ref[s] * acc[s]).astype(bf16)
        cap = weighted.shape[0]
        placer = lax.broadcasted_iota(jnp.int32, (slots, cap), 0) == place_ref[s]
        placer = jnp.where(placer, 1.0, 0.0).astype(bf16)
        placed = jnp.dot(placer, weighted, preferred_element_type=f32)
        stage[:, s] = placed.reshape(stage.shape[0], stage.shape[2], width).astype(bf16)
    ep_masks = sorted(range(1, n_ep), key=lambda m: -bin(m >> 1).count("1"))
    for mask in ep_masks:
        ret_copy(mask).start()
    back[ep] = stage[ep]

    ids = ids_ref[...]
    picker = lax.broadcasted_iota(jnp.int32, (n_tok, ids.shape[1]), 0) == ids
    picker = jnp.where(picker, 1.0, 0.0).astype(bf16)
    for mask in ep_masks:
        ret_arrived(mask)
    acc[0] = jnp.dot(picker, back[...].reshape(-1, width), preferred_element_type=f32)
    acc[0] += parts[tp].astype(f32)
    for mask in tp_masks:
        sum_copy(mask).wait_recv()
        acc[0] += parts_in[mask].astype(f32)
    out_ref[...] = acc[0].astype(bf16)

    for mask in [0] + arrivals:
        for hop in later_hops(mask, order):
            for h in (0, 1):
                hid_copy(mask, hop, h).wait_send()
    for mask in tp_masks:
        sum_copy(mask).wait_send()
    for mask in ep_masks:
        ret_copy(mask).wait_send()


def finish(n_tp, n_ep, slot_most, hidden, normed, sg, su, sd, down, gates, place, ids):
    n_tok = normed.shape[0]
    width = down.shape[2]
    n_exp, cap = gates.shape[:2]
    vmem = pl.BlockSpec(memory_space=pltpu.VMEM)
    hbm = pl.BlockSpec(memory_space=pl.ANY)
    bf16 = jnp.bfloat16
    dma = pltpu.SemaphoreType.DMA
    return pl.pallas_call(
        functools.partial(finish_kernel, n_tp, n_ep),
        out_shape=jax.ShapeDtypeStruct((n_tok, width), bf16),
        in_specs=[vmem, vmem, hbm, hbm, hbm, hbm, vmem, vmem, vmem],
        out_specs=vmem,
        scratch_shapes=[
            pltpu.VMEM(sg.shape, bf16),
            pltpu.VMEM(su.shape, bf16),
            pltpu.VMEM(sd.shape, bf16),
            pltpu.VMEM(down.shape, bf16),
            pltpu.VMEM((n_tp,) + hidden.shape, bf16),
            pltpu.VMEM((n_exp, cap, width), jnp.float32),
            pltpu.VMEM((n_tp, n_tok, width), bf16),
            pltpu.VMEM((n_tp, n_tok, width), bf16),
            pltpu.VMEM((n_ep, n_exp, slot_most, width), bf16),
            pltpu.VMEM((n_ep, n_exp, slot_most, width), bf16),
            dma((4,)),
            dma((n_tp, 2)),
            dma((n_tp, 2)),
            dma((n_tp,)),
            dma((n_tp,)),
            dma((n_ep,)),
            dma((n_ep,)),
        ],
        compiler_params=pltpu.CompilerParams(
            collective_id=1, has_side_effects=True, vmem_limit_bytes=56 * 1024 * 1024
        ),
    )(hidden, normed, sg, su, sd, down, gates, place, ids)


def on_device(
    tokens,
    norm_gain,
    shared_gate,
    shared_up,
    shared_down,
    expert_gate,
    expert_up,
    expert_down,
    chosen,
    gates,
):
    n_tp = lax.axis_size("tp")
    n_ep = lax.axis_size("ep")
    ep = lax.axis_index("ep")
    n_exp, cap = chosen.shape
    n_tok, width = tokens.shape
    f32 = jnp.float32

    sg, su, sd, own_rows, used_rows, all_chosen = upfront(
        n_tp, n_ep, tokens, shared_gate.T, shared_up.T, shared_down, chosen
    )
    sg, su, sd = flat_weight(sg), flat_weight(su), flat_weight(sd)
    all_chosen = all_chosen.reshape(-1, cap)

    slot_most = 2 * cap // n_ep
    positions = jnp.arange(cap, dtype=jnp.int32)
    sources = chosen // n_tok
    before = chosen[:, None, :] < (sources * n_tok)[:, :, None]
    run_start = jnp.sum(before.astype(jnp.int32), axis=2)
    slot_index = sources * slot_most + positions[None, :] - run_start
    first = jnp.sum((all_chosen < ep * n_tok).astype(jnp.int32), axis=1)
    stop = jnp.sum((all_chosen < (ep + 1) * n_tok).astype(jnp.int32), axis=1)
    slots = jnp.arange(slot_most, dtype=jnp.int32)
    wanted = first[:, None] + slots[None, :]
    wanted = jnp.where(wanted < stop[:, None], wanted, -1)
    own_ids = jnp.sum(
        jnp.where(
            wanted[:, :, None] == positions[None, None, :],
            (all_chosen - ep * n_tok + 1)[:, None, :],
            0,
        ),
        axis=2,
    ) - 1

    used = normalise(used_rows, norm_gain)
    gate_weight = expert_gate.reshape(expert_gate.shape[2], expert_gate.shape[3])
    up_weight = expert_up.reshape(expert_up.shape[2], expert_up.shape[3])
    gate_values = jnp.einsum("hd,rd->hr", gate_weight, used, preferred_element_type=f32)
    up_values = jnp.einsum("hd,rd->hr", up_weight, used, preferred_element_type=f32)
    part_hidden = (jax.nn.silu(gate_values) * up_values).astype(jnp.bfloat16)
    normed = normalise(own_rows, norm_gain)
    down = expert_down.reshape(n_tp, -1, width)
    return finish(
        n_tp,
        n_ep,
        slot_most,
        part_hidden,
        normed,
        sg,
        su,
        sd,
        down,
        gates[:, :, None],
        slot_index[:, None, :],
        own_ids.reshape(1, -1),
    )


def solution(mesh):
    return jax.shard_map(
        on_device,
        mesh=mesh,
        in_specs=(
            P("ep", "tp"),
            P(),
            P("ep", "tp"),
            P("ep", "tp"),
            P("tp", "ep"),
            P("tp", "ep", None, None),
            P("tp", "ep", None, None),
            P("ep", None, "tp"),
            P("ep", None),
            P("ep", None),
        ),
        out_specs=P("ep", "tp"),
        check_vma=False,
    )
```

```python
import functools

import jax
import jax.numpy as jnp
from jax import lax
from jax.experimental import pallas as pl
from jax.experimental.pallas import tpu as pltpu
from jax.sharding import PartitionSpec as P

norm_eps = 1e-06
MESH = pl.DeviceIdType.MESH


def flip(index, mask):
    bit = 1
    result = index
    while bit <= mask:
        if mask & bit:
            result = result + bit - 2 * bit * ((index // bit) % 2)
        bit *= 2
    return result


def bits_below(count):
    return [1 << i for i in range(count.bit_length() - 1)]


def half_orders(count):
    bits = bits_below(count)
    upper = bits[1:]
    return [upper + bits[:1], upper[::-1] + bits[:1]]


def later_hops(mask, order):
    last = max([i for i, b in enumerate(order) if mask & b], default=-1)
    return order[last + 1 :]


def masks_by_level(count):
    return sorted(range(1, count), key=lambda m: (bin(m).count("1"), -m))


def levels(count):
    found = {}
    for m in masks_by_level(count):
        found.setdefault(bin(m).count("1"), []).append(m)
    return [found[k] for k in sorted(found)]


def gather_kernel(
    n_tp,
    n_ep,
    tok_ref,
    sg_ref,
    su_ref,
    sd_ref,
    chosen_ref,
    ids_ref,
    sg_out,
    su_out,
    sd_out,
    own_out,
    used_out,
    ids_out,
    tok_all,
    sel,
    total,
    ep_send,
    ep_recv,
    tp_send,
    tp_recv,
    disp_send,
    disp_recv,
    local_sem,
):
    tp = lax.axis_index("tp")
    ep = lax.axis_index("ep")
    n_exp, cap = chosen_ref.shape[0], chosen_ref.shape[1]
    n_tok, width = tok_ref.shape
    split = n_tp // n_exp
    slot = tp // split
    orders = half_orders(n_ep)
    high_masks = [k * split for k in range(1, n_exp)]
    tp_bits = bits_below(n_tp)
    tp_order = tp_bits[::-1]
    tp_partners = sorted(set(tp_bits) | set(high_masks))

    barrier = pltpu.get_barrier_semaphore()
    for b in bits_below(n_ep):
        pl.semaphore_signal(barrier, inc=1, device_id={"ep": flip(ep, b)}, device_id_type=MESH)
    for b in tp_partners:
        pl.semaphore_signal(barrier, inc=1, device_id={"tp": flip(tp, b)}, device_id_type=MESH)
    pl.semaphore_wait(barrier, len(bits_below(n_ep)) + len(tp_partners))

    def block_of(out, block, rows):
        if len(out.shape) == 3:
            return out.at[block, rows, :]
        cols = out.shape[1] // n_ep
        return out.at[rows, pl.ds(pl.multiple_of(block * cols, cols), cols)]

    def sources(w):
        return [tok_ref, sg_ref, su_ref, sd_ref, ids_ref][w]

    def halves(w):
        return (0, 1) if w < 4 else (0,)

    def own_piece(w, h):
        ref = sources(w)
        if w == 4:
            return ref
        half = ref.shape[0] // 2
        return ref.at[pl.ds(h * half, half), :]

    def piece(w, block, h):
        ref = sources(w)
        if w == 4:
            return ids_out.at[block]
        half = ref.shape[0] // 2
        if w == 0:
            return tok_all.at[block, pl.ds(h * half, half), :]
        return block_of([None, sg_out, su_out, sd_out][w], block, pl.ds(h * half, half))

    def ep_copy(w, h, mask, hop):
        return pltpu.make_async_remote_copy(
            src_ref=own_piece(w, h) if mask == 0 else piece(w, flip(ep, mask), h),
            dst_ref=piece(w, flip(ep, mask), h),
            send_sem=ep_send.at[w, h, mask | hop],
            recv_sem=ep_recv.at[w, h, mask | hop],
            device_id={"ep": flip(ep, hop)},
            device_id_type=MESH,
        )

    def ep_arrival(w, h, mask):
        order = orders[h]
        hop = [b for b in order if mask & b][-1]
        dst = piece(w, flip(ep, mask), h)
        return pltpu.make_async_remote_copy(
            src_ref=dst,
            dst_ref=dst,
            send_sem=ep_send.at[w, h, mask],
            recv_sem=ep_recv.at[w, h, mask],
            device_id={"ep": flip(ep, hop)},
            device_id_type=MESH,
        )

    def ep_start(w):
        for position in range(len(orders[0])):
            for h in halves(w):
                ep_copy(w, h, 0, orders[h][position]).start()

    def ep_level(w, masks):
        for mask in masks:
            for h in halves(w):
                ep_arrival(w, h, mask).wait_recv()
                for hop in later_hops(mask, orders[h]):
                    ep_copy(w, h, mask, hop).start()

    def columns(ref, block):
        return ref.at[:, pl.ds(pl.multiple_of(block * width, width), width)]

    def tp_copy(mask, hop):
        return pltpu.make_async_remote_copy(
            src_ref=tok_ref if mask == 0 else columns(own_out, flip(tp, mask)),
            dst_ref=columns(own_out, flip(tp, mask)),
            send_sem=tp_send.at[mask | hop],
            recv_sem=tp_recv.at[mask | hop],
            device_id={"tp": flip(tp, hop)},
            device_id_type=MESH,
        )

    def used_piece(mask, h):
        rows = pl.ds(h * (cap // 2), cap // 2)
        cols = pl.ds(pl.multiple_of(flip(tp, mask) * width, width), width)
        return used_out.at[rows, cols]

    def disp_copy(mask, hop, h):
        if mask == 0:
            src = sel.at[flip(tp, hop) // split, pl.ds(h * (cap // 2), cap // 2), :]
        else:
            src = used_piece(mask, h)
        return pltpu.make_async_remote_copy(
            src_ref=src,
            dst_ref=used_piece(mask, h),
            send_sem=disp_send.at[mask | hop, h],
            recv_sem=disp_recv.at[mask | hop, h],
            device_id={"tp": flip(tp, hop)},
            device_id_type=MESH,
        )

    def disp_arrival(mask, h):
        dst = used_piece(mask, h)
        pltpu.make_async_remote_copy(
            src_ref=dst,
            dst_ref=dst,
            send_sem=disp_send.at[mask, h],
            recv_sem=disp_recv.at[mask, h],
            device_id={"tp": flip(tp, mask)},
            device_id_type=MESH,
        ).wait_recv()

    def low_hops(mask):
        low = mask % split
        return [b for b in bits_below(split) if b > low]

    def local_copies():
        items = [(0, tok_ref, tok_all.at[ep]), (6, ids_ref, ids_out.at[ep]), (1, tok_ref, columns(own_out, tp))]
        pairs = ((sg_ref, sg_out), (su_ref, su_out), (sd_ref, sd_out))
        for i, (ref, out) in enumerate(pairs):
            items.append((2 + i, ref, block_of(out, ep, pl.ds(0, ref.shape[0]))))
        return [pltpu.make_async_copy(s, d, local_sem.at[i]) for i, s, d in items]

    ep_start(0)
    for hop in tp_order:
        tp_copy(0, hop).start()
    locals_started = local_copies()
    for copy in locals_started:
        copy.start()
    ep_levels = levels(n_ep)
    ep_level(0, ep_levels[0])
    for w in (1, 2, 3, 4):
        ep_start(w)
    for masks in ep_levels[1:]:
        ep_level(0, masks)
    locals_started[0].wait()

    for s in range(n_exp):
        total[...] = jnp.zeros_like(total)

        def add_source(e, carry):
            ids = lax.broadcasted_iota(jnp.int32, (cap, n_tok), 1) + e * n_tok
            hits = jnp.where(chosen_ref[s] == ids, 1.0, 0.0).astype(jnp.bfloat16)
            total[...] += jnp.dot(hits, tok_all[e], preferred_element_type=jnp.float32)
            return carry

        lax.fori_loop(0, n_ep, add_source, 0)
        sel[s] = total[...].astype(jnp.bfloat16)

    for hop in high_masks + low_hops(0):
        for h in (0, 1):
            disp_copy(0, hop, h).start()
    own_used = pltpu.make_async_copy(sel.at[slot], columns(used_out, tp), local_sem.at[5])
    own_used.start()

    for w in (1, 2, 3, 4):
        ep_level(w, ep_levels[0])
    for mask in high_masks:
        for h in (0, 1):
            disp_arrival(mask, h)
            for hop in low_hops(mask):
                disp_copy(mask, hop, h).start()
    tp_seen = []
    for mask in sorted(range(1, n_tp), key=lambda m: [tp_order.index(b) for b in tp_order if m & b][-1]):
        last = [b for b in tp_order if mask & b][-1]
        if last == tp_order[0]:
            disp_wait(columns(own_out, flip(tp, mask)), tp_send, tp_recv, mask, tp)
            tp_seen.append(mask)
            for hop in later_hops(mask, tp_order):
                tp_copy(mask, hop).start()
    for masks in ep_levels[1:]:
        for w in (1, 2, 3, 4):
            ep_level(w, masks)
    for mask in range(1, n_tp):
        if mask not in high_masks:
            for h in (0, 1):
                disp_arrival(mask, h)
                for hop in low_hops(mask):
                    disp_copy(mask, hop, h).start()
    for mask in sorted(range(1, n_tp), key=lambda m: [tp_order.index(b) for b in tp_order if m & b][-1]):
        if mask not in tp_seen:
            disp_wait(columns(own_out, flip(tp, mask)), tp_send, tp_recv, mask, tp)
            for hop in later_hops(mask, tp_order):
                tp_copy(mask, hop).start()

    for copy in locals_started[1:]:
        copy.wait()
    own_used.wait()
    for w in range(5):
        for h in halves(w):
            for mask in range(n_ep):
                for hop in later_hops(mask, orders[h]):
                    ep_copy(w, h, mask, hop).wait_send()
    for mask in range(n_tp):
        for hop in later_hops(mask, tp_order):
            tp_copy(mask, hop).wait_send()
    for mask in [0] + high_masks + [m for m in range(1, n_tp) if m not in high_masks]:
        hops = low_hops(mask)
        if mask == 0:
            hops = high_masks + hops
        for hop in hops:
            for h in (0, 1):
                disp_copy(mask, hop, h).wait_send()


def disp_wait(dst, send_sem, recv_sem, mask, tp):
    pltpu.make_async_remote_copy(
        src_ref=dst,
        dst_ref=dst,
        send_sem=send_sem.at[mask],
        recv_sem=recv_sem.at[mask],
        device_id={"tp": flip(tp, mask)},
        device_id_type=MESH,
    ).wait_recv()


def upfront(n_tp, n_ep, tokens, shared_gate, shared_up, shared_down, chosen):
    n_tok, width = tokens.shape
    n_exp, cap = chosen.shape
    vmem = pl.BlockSpec(memory_space=pltpu.VMEM)
    hbm = pl.BlockSpec(memory_space=pl.ANY)
    bf16 = jnp.bfloat16

    def joined(weight):
        rows, cols = weight.shape
        if cols % 128 == 0:
            return jax.ShapeDtypeStruct((rows, n_ep * cols), bf16)
        return jax.ShapeDtypeStruct((n_ep, rows, cols), bf16)

    return pl.pallas_call(
        functools.partial(gather_kernel, n_tp, n_ep),
        out_shape=(
            joined(shared_gate),
            joined(shared_up),
            joined(shared_down),
            jax.ShapeDtypeStruct((n_tok, n_tp * width), bf16),
            jax.ShapeDtypeStruct((cap, n_tp * width), bf16),
            jax.ShapeDtypeStruct((n_ep, n_exp, cap), jnp.int32),
        ),
        in_specs=[vmem] + [hbm] * 3 + [vmem] * 2,
        out_specs=(hbm,) * 5 + (vmem,),
        scratch_shapes=[
            pltpu.VMEM((n_ep, n_tok, width), bf16),
            pltpu.VMEM((n_exp, cap, width), bf16),
            pltpu.VMEM((cap, width), jnp.float32),
            pltpu.SemaphoreType.DMA((5, 2, n_ep)),
            pltpu.SemaphoreType.DMA((5, 2, n_ep)),
            pltpu.SemaphoreType.DMA((n_tp,)),
            pltpu.SemaphoreType.DMA((n_tp,)),
            pltpu.SemaphoreType.DMA((n_tp, 2)),
            pltpu.SemaphoreType.DMA((n_tp, 2)),
            pltpu.SemaphoreType.DMA((7,)),
        ],
        compiler_params=pltpu.CompilerParams(
            collective_id=0, has_side_effects=True, vmem_limit_bytes=48 * 1024 * 1024
        ),
    )(tokens, shared_gate, shared_up, shared_down, chosen[:, :, None], chosen)


def flat_weight(weight):
    if weight.ndim == 2:
        return weight
    return jnp.moveaxis(weight, 0, 1).reshape(weight.shape[1], -1)


def normalise(rows, gain):
    widened = rows.astype(jnp.float32)
    inv_scale = lax.rsqrt(jnp.mean(widened * widened, axis=1, keepdims=True) + norm_eps)
    return (widened * inv_scale * gain).astype(jnp.bfloat16)


def finish_kernel(
    n_tp,
    n_ep,
    part_ref,
    normed_ref,
    sg_hbm,
    su_hbm,
    sd_hbm,
    down_hbm,
    gates_ref,
    place_ref,
    ids_ref,
    out_ref,
    sg_ref,
    su_ref,
    sd_ref,
    down_ref,
    hidden,
    acc,
    parts,
    parts_in,
    stage,
    back,
    load_sem,
    hid_send,
    hid_recv,
    sum_send,
    sum_recv,
    ret_send,
    ret_recv,
):
    tp = lax.axis_index("tp")
    ep = lax.axis_index("ep")
    n_tok, width = out_ref.shape
    n_exp = gates_ref.shape[0]
    split = n_tp // n_exp
    f32, bf16 = jnp.float32, jnp.bfloat16
    order = bits_below(n_tp)[::-1]
    half = part_ref.shape[0] // 2

    barrier = pltpu.get_barrier_semaphore()
    for mask in range(1, n_tp):
        pl.semaphore_signal(barrier, inc=1, device_id={"tp": flip(tp, mask)}, device_id_type=MESH)
    for mask in range(1, n_ep):
        pl.semaphore_signal(barrier, inc=1, device_id={"ep": flip(ep, mask)}, device_id_type=MESH)
    pl.semaphore_wait(barrier, n_tp + n_ep - 2)

    def hid_copy(mask, hop, h):
        rows = pl.ds(h * half, half)
        block = flip(tp, mask)
        return pltpu.make_async_remote_copy(
            src_ref=part_ref.at[rows, :] if mask == 0 else hidden.at[block, rows, :],
            dst_ref=hidden.at[block, rows, :],
            send_sem=hid_send.at[mask | hop, h],
            recv_sem=hid_recv.at[mask | hop, h],
            device_id={"tp": flip(tp, hop)},
            device_id_type=MESH,
        )

    def hid_arrived(mask, h):
        dst = hidden.at[flip(tp, mask), pl.ds(h * half, half), :]
        pltpu.make_async_remote_copy(
            src_ref=dst,
            dst_ref=dst,
            send_sem=hid_send.at[mask, h],
            recv_sem=hid_recv.at[mask, h],
            device_id={"tp": flip(tp, mask)},
            device_id_type=MESH,
        ).wait_recv()

    def sum_copy(mask):
        return pltpu.make_async_remote_copy(
            src_ref=parts.at[flip(tp, mask)],
            dst_ref=parts_in.at[mask],
            send_sem=sum_send.at[mask],
            recv_sem=sum_recv.at[mask],
            device_id={"tp": flip(tp, mask)},
            device_id_type=MESH,
        )

    def ret_copy(mask):
        return pltpu.make_async_remote_copy(
            src_ref=stage.at[flip(ep, mask)],
            dst_ref=back.at[ep],
            send_sem=ret_send.at[mask],
            recv_sem=ret_recv.at[mask],
            device_id={"ep": flip(ep, mask)},
            device_id_type=MESH,
        )

    def ret_arrived(mask):
        dst = back.at[flip(ep, mask)]
        pltpu.make_async_remote_copy(
            src_ref=dst,
            dst_ref=dst,
            send_sem=ret_send.at[mask],
            recv_sem=ret_recv.at[mask],
            device_id={"ep": flip(ep, mask)},
            device_id_type=MESH,
        ).wait_recv()

    for hop in order:
        for h in (0, 1):
            hid_copy(0, hop, h).start()
    pairs = ((sg_hbm, sg_ref), (su_hbm, su_ref), (sd_hbm, sd_ref), (down_hbm, down_ref))
    loads = [pltpu.make_async_copy(s, d, load_sem.at[i]) for i, (s, d) in enumerate(pairs)]
    for load in loads:
        load.start()

    for load in loads[:3]:
        load.wait()
    chunk = n_tok // 2

    def shared_rows(i, carry):
        rows = pl.ds(pl.multiple_of(i * chunk, chunk), chunk)
        x = normed_ref[rows, :]
        contract = (((1,), (1,)), ((), ()))
        gate = lax.dot_general(x, sg_ref[...], contract, preferred_element_type=f32)
        up = lax.dot_general(x, su_ref[...], contract, preferred_element_type=f32)
        mid = (jax.nn.silu(gate) * up).astype(bf16)
        for block in range(n_tp):
            cols = pl.ds(block * width, width)
            parts[block, rows, :] = jnp.dot(
                mid, sd_ref[:, cols], preferred_element_type=f32
            ).astype(bf16)
        return carry

    lax.fori_loop(0, 2, shared_rows, 0)
    loads[3].wait()

    acc[...] = jnp.zeros_like(acc)

    def add_block(mask):
        block = flip(tp, mask)
        value = part_ref[...] if mask == 0 else hidden[block]
        slot = block // split
        acc[slot] += lax.dot_general(
            value, down_ref[block], (((0,), (0,)), ((), ())), preferred_element_type=f32
        )

    arrivals = sorted(
        range(1, n_tp), key=lambda m: [order.index(b) for b in order if m & b][::-1]
    )
    tp_masks = list(range(1, n_tp))
    first_hop = [m for m in arrivals if m == order[0]]
    for mask in first_hop:
        for h in (0, 1):
            hid_arrived(mask, h)
            for hop in later_hops(mask, order):
                hid_copy(mask, hop, h).start()
    for mask in tp_masks:
        sum_copy(mask).start()
    add_block(0)
    for mask in first_hop:
        add_block(mask)
    for mask in arrivals:
        if mask in first_hop:
            continue
        for h in (0, 1):
            hid_arrived(mask, h)
            for hop in later_hops(mask, order):
                hid_copy(mask, hop, h).start()
        add_block(mask)

    slots = stage.shape[0] * stage.shape[2]
    for s in range(n_exp):
        weighted = (gates_ref[s] * acc[s]).astype(bf16)
        cap = weighted.shape[0]
        placer = lax.broadcasted_iota(jnp.int32, (slots, cap), 0) == place_ref[s]
        placer = jnp.where(placer, 1.0, 0.0).astype(bf16)
        placed = jnp.dot(placer, weighted, preferred_element_type=f32)
        stage[:, s] = placed.reshape(stage.shape[0], stage.shape[2], width).astype(bf16)
    ep_masks = sorted(range(1, n_ep), key=lambda m: -bin(m >> 1).count("1"))
    for mask in ep_masks:
        ret_copy(mask).start()
    back[ep] = stage[ep]

    ids = ids_ref[...]
    picker = lax.broadcasted_iota(jnp.int32, (n_tok, ids.shape[1]), 0) == ids
    picker = jnp.where(picker, 1.0, 0.0).astype(bf16)
    for mask in ep_masks:
        ret_arrived(mask)
    acc[0] = jnp.dot(picker, back[...].reshape(-1, width), preferred_element_type=f32)
    acc[0] += parts[tp].astype(f32)
    for mask in tp_masks:
        sum_copy(mask).wait_recv()
        acc[0] += parts_in[mask].astype(f32)
    out_ref[...] = acc[0].astype(bf16)

    for mask in [0] + arrivals:
        for hop in later_hops(mask, order):
            for h in (0, 1):
                hid_copy(mask, hop, h).wait_send()
    for mask in tp_masks:
        sum_copy(mask).wait_send()
    for mask in ep_masks:
        ret_copy(mask).wait_send()


def finish(n_tp, n_ep, slot_most, hidden, normed, sg, su, sd, down, gates, place, ids):
    n_tok = normed.shape[0]
    width = down.shape[2]
    n_exp, cap = gates.shape[:2]
    vmem = pl.BlockSpec(memory_space=pltpu.VMEM)
    hbm = pl.BlockSpec(memory_space=pl.ANY)
    bf16 = jnp.bfloat16
    dma = pltpu.SemaphoreType.DMA
    return pl.pallas_call(
        functools.partial(finish_kernel, n_tp, n_ep),
        out_shape=jax.ShapeDtypeStruct((n_tok, width), bf16),
        in_specs=[vmem, vmem, hbm, hbm, hbm, hbm, vmem, vmem, vmem],
        out_specs=vmem,
        scratch_shapes=[
            pltpu.VMEM(sg.shape, bf16),
            pltpu.VMEM(su.shape, bf16),
            pltpu.VMEM(sd.shape, bf16),
            pltpu.VMEM(down.shape, bf16),
            pltpu.VMEM((n_tp,) + hidden.shape, bf16),
            pltpu.VMEM((n_exp, cap, width), jnp.float32),
            pltpu.VMEM((n_tp, n_tok, width), bf16),
            pltpu.VMEM((n_tp, n_tok, width), bf16),
            pltpu.VMEM((n_ep, n_exp, slot_most, width), bf16),
            pltpu.VMEM((n_ep, n_exp, slot_most, width), bf16),
            dma((4,)),
            dma((n_tp, 2)),
            dma((n_tp, 2)),
            dma((n_tp,)),
            dma((n_tp,)),
            dma((n_ep,)),
            dma((n_ep,)),
        ],
        compiler_params=pltpu.CompilerParams(
            collective_id=1, has_side_effects=True, vmem_limit_bytes=56 * 1024 * 1024
        ),
    )(hidden, normed, sg, su, sd, down, gates, place, ids)


def on_device(
    tokens,
    norm_gain,
    shared_gate,
    shared_up,
    shared_down,
    expert_gate,
    expert_up,
    expert_down,
    chosen,
    gates,
):
    n_tp = lax.axis_size("tp")
    n_ep = lax.axis_size("ep")
    ep = lax.axis_index("ep")
    n_exp, cap = chosen.shape
    n_tok, width = tokens.shape
    f32 = jnp.float32

    sg, su, sd, own_rows, used_rows, all_chosen = upfront(
        n_tp, n_ep, tokens, shared_gate.T, shared_up.T, shared_down, chosen
    )
    sg, su, sd = flat_weight(sg), flat_weight(su), flat_weight(sd)
    all_chosen = all_chosen.reshape(-1, cap)

    slot_most = 2 * cap // n_ep
    positions = jnp.arange(cap, dtype=jnp.int32)
    sources = chosen // n_tok
    before = chosen[:, None, :] < (sources * n_tok)[:, :, None]
    run_start = jnp.sum(before.astype(jnp.int32), axis=2)
    slot_index = sources * slot_most + positions[None, :] - run_start
    first = jnp.sum((all_chosen < ep * n_tok).astype(jnp.int32), axis=1)
    stop = jnp.sum((all_chosen < (ep + 1) * n_tok).astype(jnp.int32), axis=1)
    slots = jnp.arange(slot_most, dtype=jnp.int32)
    wanted = first[:, None] + slots[None, :]
    wanted = jnp.where(wanted < stop[:, None], wanted, -1)
    own_ids = jnp.sum(
        jnp.where(
            wanted[:, :, None] == positions[None, None, :],
            (all_chosen - ep * n_tok + 1)[:, None, :],
            0,
        ),
        axis=2,
    ) - 1

    used = normalise(used_rows, norm_gain)
    gate_weight = expert_gate.reshape(expert_gate.shape[2], expert_gate.shape[3])
    up_weight = expert_up.reshape(expert_up.shape[2], expert_up.shape[3])
    gate_values = jnp.einsum("hd,rd->hr", gate_weight, used, preferred_element_type=f32)
    up_values = jnp.einsum("hd,rd->hr", up_weight, used, preferred_element_type=f32)
    part_hidden = (jax.nn.silu(gate_values) * up_values).astype(jnp.bfloat16)
    normed = normalise(own_rows, norm_gain)
    down = expert_down.reshape(n_tp, -1, width)
    return finish(
        n_tp,
        n_ep,
        slot_most,
        part_hidden,
        normed,
        sg,
        su,
        sd,
        down,
        gates[:, :, None],
        slot_index[:, None, :],
        own_ids.reshape(1, -1),
    )


def solution(mesh):
    return jax.shard_map(
        on_device,
        mesh=mesh,
        in_specs=(
            P("ep", "tp"),
            P(),
            P("ep", "tp"),
            P("ep", "tp"),
            P("tp", "ep"),
            P("tp", "ep", None, None),
            P("tp", "ep", None, None),
            P("ep", None, "tp"),
            P("ep", None),
            P("ep", None),
        ),
        out_specs=P("ep", "tp"),
        check_vma=False,
    )
```
